256 devices in a mesh: scen: 32 (over y, x, core), row: 4 (over z_hi), col: 2 (over z_lo).
Axes of the slice: x: 4, y: 4, z: 8 (z_hi: 4, z_lo: 2; z = z_hi * 2 + z_lo), core: 2. Of those that a mesh axis runs over, the one named last changes fastest.
Arguments:
- border: bfloat16 [128, 32, 512, 512], P('scen', None, ('row', 'col')), may hold values from -4.5 to 4.5, as said below
- panel_border: bfloat16 [128, 512, 512], P('scen'), may hold values from -0.09375 to 0.09375
- kinv: bfloat16 [128, 512, 512], P('scen'), may hold values from -1 to 4, as said below
- factor: bfloat16 [16384, 4096], P(('scen', 'row'), 'col'), may hold values from -4.5 to 4.5
- root_block: float32 [16384, 512], P(('scen', 'row', 'col')), may hold values from -9 to 43, as said below
Outputs:
- panel_factor: float32 [16384, 512], P(('scen', 'row', 'col'))
The draws below stay inside these ranges and needn't reach their ends.
Inputs may be any that keep to these rules, and one draw needn't show every extreme that they name: border[s, 0] is panel_border[s] transposed. `kinv`: each scenario's matrix is symmetric positive definite up to rounding, with eigenvalues 0.5 or more. `root_block`: its first 512 rows form a symmetric matrix; schur[0:512] is positive definite.
All inputs are finite; a program needn't handle non-finite values.
Results may differ from the reference program's by a relative error of at most 0.0025.
Values may be sent and summed in bfloat16 or wider, within the bound.
No kernel may reach another device: no remote copies, remote signals or barrier semaphores. Data moves between devices by JAX's collectives and lax.ppermute only.
A program may use at most 128 MiB of HBM per device.

```python
import jax
import jax.numpy as jnp
from jax import lax

NS = 512
PANEL = 512
KRES = 4096
SCEN = 128
ROWS = 16384
N_SCEN = 32


def panel_columns(key):
    base = jnp.clip(jax.random.normal(jax.random.fold_in(key, 7), (SCEN, NS, PANEL), jnp.float32), -6.0, 6.0)
    return base * (SCEN * NS / 16.0) ** (-0.5)


def draw_panel_border(key, part):
    return panel_columns(key).astype(jnp.bfloat16)


def draw_border(key, part):
    base = jnp.clip(jax.random.normal(jax.random.fold_in(key, 11), (SCEN, N_SCEN, PANEL, NS), jnp.float32), -6.0, 6.0) * 0.75
    own = jnp.transpose(panel_columns(key), (0, 2, 1))
    return base.at[:, 0].set(own).astype(jnp.bfloat16)


def draw_kinv(key, part):
    base = jax.random.normal(key, (SCEN, NS, NS), jnp.float32)
    gram = jnp.einsum('snk,smk->snm', base, base, precision=lax.Precision.HIGHEST) / (2.0 * NS)
    return (gram + 0.5 * jnp.eye(NS, dtype=jnp.float32)).astype(jnp.bfloat16)


def draw_factor(key, part):
    base = jnp.clip(jax.random.normal(key, (ROWS, KRES), jnp.float32), -6.0, 6.0)
    places = lax.broadcasted_iota(jnp.int32, (ROWS, 1), 0)
    scales = jnp.where(places < PANEL, 2.0 / KRES ** 0.5, 0.75)
    return (base * scales).astype(jnp.bfloat16)


def draw_root_block(key, part):
    base = jnp.clip(jax.random.normal(key, (ROWS, PANEL), jnp.float32), -6.0, 6.0)
    square = base[0:PANEL]
    block = (square + square.T) * 0.212 + 40.0 * jnp.eye(PANEL, dtype=jnp.float32)
    return jnp.concatenate([block, 1.5 * base[PANEL:]], axis=0)


def setup_inputs(seed: int = 0) -> dict:
    splits = jax.random.split(jax.random.key(seed), 6)
    border = draw_border(jax.random.fold_in(splits[5], 71), 0)
    panel_border = draw_panel_border(jax.random.fold_in(splits[5], 71), 0)
    kinv = draw_kinv(jax.random.fold_in(splits[5], 71), 0)
    factor = draw_factor(jax.random.fold_in(splits[5], 71), 0)
    root_block = draw_root_block(jax.random.fold_in(splits[5], 71), 0)
    return dict(border=border, panel_border=panel_border, kinv=kinv, factor=factor, root_block=root_block)


def reference(border, panel_border, kinv, factor, root_block):
    slab = border.reshape(SCEN, ROWS, NS)

    def add_scenario(total, items):
        rows_part, panel_part, inverse = items
        solved = jnp.dot(inverse.astype(jnp.float32), panel_part.astype(jnp.float32), preferred_element_type=jnp.float32).astype(jnp.bfloat16)
        return (total + jnp.dot(rows_part.astype(jnp.float32), solved.astype(jnp.float32), preferred_element_type=jnp.float32), None)
    coupling, unused = lax.scan(add_scenario, jnp.zeros((ROWS, PANEL), jnp.float32), (slab, panel_border, kinv))
    leading = factor[0:PANEL]
    update = lax.dot_general(factor.astype(jnp.float32), leading.astype(jnp.float32), (((1,), (1,)), ((), ())), preferred_element_type=jnp.float32)
    schur = root_block + coupling - update
    lower = jnp.linalg.cholesky(schur[0:PANEL])
    return jax.scipy.linalg.solve_triangular(lower, schur.T, lower=True).T
```

```python
import jax
import jax.numpy as jnp
from jax import lax
from jax.experimental import pallas as pl
from jax.experimental.pallas import tpu as pltpu
from jax.sharding import Mesh
from jax.sharding import PartitionSpec as P

CHIPS = ("scen_0", "scen_1")
CORE = "scen_2"
SCEN = ("scen_0", "scen_1", "scen_2")
SCEN_ROW = ("scen_0", "scen_1", "scen_2", "row")
SCEN_ROW_COL = ("scen_0", "scen_1", "scen_2", "row", "col")
BF16 = jnp.bfloat16

BLOCK = 128
F32 = jnp.float32


def spread_row(value, row):
    return jnp.broadcast_to(value[row : row + 1, :], value.shape)


def spread_lane(value, lane):
    return jnp.broadcast_to(value[:, lane : lane + 1], value.shape)


def factor_block(rows):
    groups = len(rows)
    tile = rows[0].shape
    sub = lax.broadcasted_iota(jnp.int32, tile, 0)
    lane = lax.broadcasted_iota(jnp.int32, tile, 1)
    inverse = [jnp.where(lane == sub + 8 * g, 1.0, 0.0).astype(F32) for g in range(groups)]
    rows = list(rows)
    done = []
    for t in range(groups):
        cols = [spread_lane(rows[t], 8 * t + j) for j in range(8)]
        left, right = rows[t], inverse[t]
        ahead = inverse[t]
        scale = jnp.zeros(tile, F32)
        square = jnp.zeros(tile, F32)
        for k in range(8):
            root = lax.rsqrt(spread_row(cols[k], k))
            recip = root * root
            scale = jnp.where(sub == k, root, scale)
            square = jnp.where(sub == k, recip, square)
            full = jnp.where(sub == k, 0.0, cols[k] * recip)
            below = jnp.where(sub > k, full, 0.0)
            for j in range(k + 1, 8):
                cols[j] = cols[j] - full * spread_row(cols[j], k)
            left = left - full * spread_row(left, k)
            right = right - full * spread_row(right, k)
            ahead = ahead - below * spread_row(ahead, k)
        done.append(ahead * scale)
        if t == groups - 1:
            break
        left, right = left * square, right * square
        lefts = [spread_row(left, j) for j in range(8)]
        rights = [spread_row(right, j) for j in range(8)]
        for g in range(t + 1, groups):
            coef = [spread_lane(rows[g], 8 * t + j) for j in range(8)]
            a = [coef[j] * lefts[j] for j in range(8)]
            b = [coef[j] * rights[j] for j in range(8)]
            while len(a) > 1:
                a = [a[i] + a[i + 1] for i in range(0, len(a), 2)]
                b = [b[i] + b[i + 1] for i in range(0, len(b), 2)]
            rows[g] = rows[g] - a[0]
            inverse[g] = inverse[g] - b[0]
    return done


def dot(a, b, dims=((1,), (0,))):
    return lax.dot_general(a, b, (dims, ((), ())), precision=lax.Precision.HIGHEST, preferred_element_type=F32)


def inverse_kernel(core_ref, own_ref, other_ref, w_ref, s_ref, d_ref):
    n = w_ref.shape[0]
    blocks = n // BLOCK
    planes = own_ref.shape[1]
    half = n // planes // 2
    own = pl.multiple_of(core_ref[0] * half, half)
    other = pl.multiple_of(half - core_ref[0] * half, half)
    for piece in range(own_ref.shape[0]):
        down, across = divmod(piece, n // BLOCK)
        for plane in range(planes):
            at = plane * 2 * half + down * 8
            lanes = slice(across * BLOCK, (across + 1) * BLOCK)
            s_ref[pl.ds(own + at, 8), lanes] = own_ref[piece, plane]
            s_ref[pl.ds(other + at, 8), lanes] = other_ref[piece, plane]
    for k in range(blocks):
        lo, hi = k * BLOCK, (k + 1) * BLOCK
        done = factor_block([s_ref[lo + 8 * g : lo + 8 * g + 8, lo:hi] for g in range(BLOCK // 8)])
        for g in range(BLOCK // 8):
            d_ref[8 * g : 8 * g + 8, :] = done[g]
        w = d_ref[...]
        if k > 0:
            w_ref[lo:hi, 0:lo] = dot(w, w_ref[lo:hi, 0:lo])
        w_ref[lo:hi, lo:hi] = w
        if hi < n:
            w_ref[lo:hi, hi:n] = jnp.zeros((BLOCK, n - hi), F32)
            u = dot(w, s_ref[lo:hi, hi:n])
            for i in range(k + 1, blocks):
                il, ih = i * BLOCK, (i + 1) * BLOCK
                ui = u[:, il - hi : ih - hi]
                s_ref[il:ih, il:n] = s_ref[il:ih, il:n] - dot(ui, u[:, il - hi :], ((0,), (0,)))
                new = dot(ui, w_ref[lo:hi, 0:hi], ((0,), (0,)))
                if k > 0:
                    w_ref[il:ih, 0:lo] = w_ref[il:ih, 0:lo] - new[:, 0:lo]
                w_ref[il:ih, lo:hi] = -new[:, lo:hi]


def inverse_factor(core, own, other, n):
    return pl.pallas_call(
        inverse_kernel,
        out_shape=jax.ShapeDtypeStruct((n, n), F32),
        in_specs=[
            pl.BlockSpec(memory_space=pltpu.SMEM),
            pl.BlockSpec(memory_space=pltpu.VMEM),
            pl.BlockSpec(memory_space=pltpu.VMEM),
        ],
        out_specs=pl.BlockSpec(memory_space=pltpu.VMEM),
        scratch_shapes=[pltpu.VMEM((n, n), F32), pltpu.VMEM((BLOCK, BLOCK), F32)],
        cost_estimate=pl.CostEstimate(flops=40_000_000, bytes_accessed=2 * n * n * 4, transcendentals=n),
        name="inverse_factor",
    )(core, own, other)


def swapped(value, axis):
    return lax.ppermute(value, axis, [(0, 1), (1, 0)])


def gathered(value, axis):
    peers = lax.axis_size(axis)
    place = lax.axis_index(axis)
    pieces = [value]
    for step in range(1, peers):
        pieces.append(lax.ppermute(value, axis, [(i, (i + step) % peers) for i in range(peers)]))
    pieces = jnp.stack(pieces)
    return jnp.stack(
        [lax.dynamic_index_in_dim(pieces, (place - q) % peers, 0, keepdims=False) for q in range(peers)]
    )


def all_planes(value):
    pieces = gathered(gathered(value, "col"), "row")
    return pieces.reshape(-1, *value.shape)


def exchanged(pieces, axis):
    return lax.all_to_all(pieces, axis, 0, 0, tiled=True)


def half_of(value, dim, which, parts=2):
    size = value.shape[dim] // parts
    return lax.dynamic_slice_in_dim(value, which * size, size, dim)


def factor_slices(factor):
    col = lax.axis_index("col")
    chips = lax.axis_size(SCEN) // 2
    mine = half_of(factor, 0, col)
    theirs = swapped(half_of(factor, 0, 1 - col), "col")
    mine, theirs = (
        jnp.moveaxis(v.reshape(v.shape[0], chips, -1), 1, 0) for v in (mine, theirs)
    )
    first = jnp.where(col == 0, mine, theirs)
    second = jnp.where(col == 0, theirs, mine)
    return exchanged(jnp.concatenate([first, second]), SCEN)


def per_device(border, panel_border, kinv, factor, root_block):
    core = lax.axis_index(CORE)
    scen = lax.axis_index(SCEN)
    plane = lax.axis_index(("row", "col"))
    chips = lax.axis_size(CHIPS)
    groups, rows, n = border.shape[1], border.shape[2], border.shape[3]

    slices = factor_slices(factor)
    leading = all_planes(slices[0])
    leading = leading.reshape(-1, leading.shape[-1])

    solved = jnp.einsum(
        "snm,smp->snp", kinv, panel_border, preferred_element_type=F32
    ).astype(BF16)

    own_solved = lax.dynamic_slice_in_dim(solved, plane * rows, rows, 2)
    panel = jnp.einsum("snr,snp->rp", own_solved, panel_border, preferred_element_type=F32)
    panel = panel - lax.dot_general(
        slices[0], leading, (((1,), (1,)), ((), ())), preferred_element_type=F32
    )
    panel = panel + jnp.where(scen == 0, root_block, 0.0)
    panel = half_of(panel, 0, core) + swapped(half_of(panel, 0, 1 - core), CORE)
    width = panel.shape[1]
    tiles = panel.reshape(panel.shape[0] // 8, 8, width // BLOCK, BLOCK)
    tiles = tiles.transpose(0, 2, 1, 3).reshape(-1, 8, BLOCK)
    tile = jnp.sum(exchanged(tiles, CHIPS), axis=0)
    tile = all_planes(tile)
    own = exchanged(jnp.broadcast_to(tile, (chips, *tile.shape)), CHIPS)
    other = swapped(own, CORE)
    inverse = inverse_factor(core.astype(jnp.int32).reshape(1), own, other, width)

    coupling = jnp.einsum("sgrn,snp->grp", border, solved, preferred_element_type=F32)
    update = lax.dot_general(
        slices, leading, (((2,), (1,)), ((), ())), preferred_element_type=F32
    )
    partial = (coupling - update).reshape(chips, 2, rows, width)
    mine = half_of(partial, 1, core)[:, 0] + swapped(half_of(partial, 1, 1 - core), CORE)[:, 0]
    pieces = exchanged(mine.astype(BF16), CHIPS)
    schur = root_block + jnp.sum(pieces.astype(F32), axis=0)
    return lax.dot_general(
        schur, inverse, (((1,), (1,)), ((), ())),
        precision=lax.Precision.HIGHEST, preferred_element_type=F32,
    )


def solution(mesh):
    split = Mesh(
        mesh.devices.reshape(4, 4, 2, mesh.shape["row"], mesh.shape["col"]),
        ("scen_0", "scen_1", "scen_2", "row", "col"),
    )
    in_specs = (
        P(SCEN, None, ("row", "col"), None),
        P(SCEN, None, None),
        P(SCEN, None, None),
        P(SCEN_ROW, "col"),
        P(SCEN_ROW_COL, None),
    )
    out_specs = P(SCEN_ROW_COL, None)
    return jax.shard_map(
        per_device, mesh=split, in_specs=in_specs, out_specs=out_specs, check_vma=False
    )
```

```python
import jax
import jax.numpy as jnp
import numpy as np
from jax import lax
from jax.experimental import pallas as pl
from jax.experimental.pallas import tpu as pltpu
from jax.sharding import Mesh
from jax.sharding import PartitionSpec as P

CHIPS = ("scen_0", "scen_1")
CORE = "scen_2"
SCEN = ("scen_0", "scen_1", "scen_2")
SCEN_ROW = ("scen_0", "scen_1", "scen_2", "row")
SCEN_ROW_COL = ("scen_0", "scen_1", "scen_2", "row", "col")
BF16 = jnp.bfloat16

BLOCK = 128
F32 = jnp.float32


def spread_row(value, row):
    return jnp.broadcast_to(value[row : row + 1, :], value.shape)


def spread_lane(value, lane):
    return jnp.broadcast_to(value[:, lane : lane + 1], value.shape)


def factor_block(rows):
    groups = len(rows)
    tile = rows[0].shape
    sub = lax.broadcasted_iota(jnp.int32, tile, 0)
    lane = lax.broadcasted_iota(jnp.int32, tile, 1)
    inverse = [jnp.where(lane == sub + 8 * g, 1.0, 0.0).astype(F32) for g in range(groups)]
    rows = list(rows)
    done = []
    for t in range(groups):
        cols = [spread_lane(rows[t], 8 * t + j) for j in range(8)]
        left, right = rows[t], inverse[t]
        ahead = inverse[t]
        scale = jnp.zeros(tile, F32)
        square = jnp.zeros(tile, F32)
        for k in range(8):
            root = lax.rsqrt(spread_row(cols[k], k))
            recip = root * root
            scale = jnp.where(sub == k, root, scale)
            square = jnp.where(sub == k, recip, square)
            full = jnp.where(sub == k, 0.0, cols[k] * recip)
            below = jnp.where(sub > k, full, 0.0)
            for j in range(k + 1, 8):
                cols[j] = cols[j] - full * spread_row(cols[j], k)
            left = left - full * spread_row(left, k)
            right = right - full * spread_row(right, k)
            ahead = ahead - below * spread_row(ahead, k)
        done.append(ahead * scale)
        if t == groups - 1:
            break
        left, right = left * square, right * square
        lefts = [spread_row(left, j) for j in range(8)]
        rights = [spread_row(right, j) for j in range(8)]
        for g in range(t + 1, groups):
            coef = [spread_lane(rows[g], 8 * t + j) for j in range(8)]
            a = [coef[j] * lefts[j] for j in range(8)]
            b = [coef[j] * rights[j] for j in range(8)]
            while len(a) > 1:
                a = [a[i] + a[i + 1] for i in range(0, len(a), 2)]
                b = [b[i] + b[i + 1] for i in range(0, len(b), 2)]
            rows[g] = rows[g] - a[0]
            inverse[g] = inverse[g] - b[0]
    return done


def dot(a, b, dims=((1,), (0,))):
    return lax.dot_general(a, b, (dims, ((), ())), precision=lax.Precision.HIGHEST, preferred_element_type=F32)


def inverse_kernel(place_ref, own_ref, other_ref, w_ref, s_ref, d_ref):
    n = w_ref.shape[0]
    blocks = n // BLOCK
    planes, half = own_ref.shape[0], own_ref.shape[1]
    for piece in range(planes):
        own = pl.multiple_of(place_ref[0, piece], half)
        other = pl.multiple_of(place_ref[1, piece], half)
        s_ref[pl.ds(own, half), :] = own_ref[piece]
        s_ref[pl.ds(other, half), :] = other_ref[piece]
    for k in range(blocks):
        lo, hi = k * BLOCK, (k + 1) * BLOCK
        done = factor_block([s_ref[lo + 8 * g : lo + 8 * g + 8, lo:hi] for g in range(BLOCK // 8)])
        for g in range(BLOCK // 8):
            d_ref[8 * g : 8 * g + 8, :] = done[g]
        w = d_ref[...]
        if k > 0:
            w_ref[lo:hi, 0:lo] = dot(w, w_ref[lo:hi, 0:lo])
        w_ref[lo:hi, lo:hi] = w
        if hi < n:
            w_ref[lo:hi, hi:n] = jnp.zeros((BLOCK, n - hi), F32)
            u = dot(w, s_ref[lo:hi, hi:n])
            for i in range(k + 1, blocks):
                il, ih = i * BLOCK, (i + 1) * BLOCK
                ui = u[:, il - hi : ih - hi]
                s_ref[il:ih, il:n] = s_ref[il:ih, il:n] - dot(ui, u[:, il - hi :], ((0,), (0,)))
                new = dot(ui, w_ref[lo:hi, 0:hi], ((0,), (0,)))
                if k > 0:
                    w_ref[il:ih, 0:lo] = w_ref[il:ih, 0:lo] - new[:, 0:lo]
                w_ref[il:ih, lo:hi] = -new[:, lo:hi]


def inverse_factor(place, own, other):
    n = own.shape[-1]
    return pl.pallas_call(
        inverse_kernel,
        out_shape=jax.ShapeDtypeStruct((n, n), F32),
        in_specs=[
            pl.BlockSpec(memory_space=pltpu.SMEM),
            pl.BlockSpec(memory_space=pltpu.VMEM),
            pl.BlockSpec(memory_space=pltpu.VMEM),
        ],
        out_specs=pl.BlockSpec(memory_space=pltpu.VMEM),
        scratch_shapes=[pltpu.VMEM((n, n), F32), pltpu.VMEM((BLOCK, BLOCK), F32)],
        cost_estimate=pl.CostEstimate(flops=40_000_000, bytes_accessed=2 * n * n * 4, transcendentals=n),
        name="inverse_factor",
    )(place, own, other)


def swapped(value, axis):
    return lax.ppermute(value, axis, [(0, 1), (1, 0)])


def gathered(value, axis):
    peers = lax.axis_size(axis)
    place = lax.axis_index(axis)
    pieces = [value]
    for step in range(1, peers):
        pieces.append(lax.ppermute(value, axis, [(i, (i + step) % peers) for i in range(peers)]))
    pieces = jnp.stack(pieces)
    return jnp.stack(
        [lax.dynamic_index_in_dim(
                pieces, lax.rem(place + (peers - q), peers), 0, keepdims=False
            ) for q in range(peers)]
    )


def all_planes(value):
    pieces = gathered(gathered(value, "col"), "row")
    return pieces.reshape(-1, *value.shape)


def shifts(value, axis):
    peers = lax.axis_size(axis)
    return [value] + [
        lax.ppermute(value, axis, [(i, (i + step) % peers) for i in range(peers)])
        for step in range(1, peers)
    ]


def plane_pieces(value):
    pairs = jnp.stack([value, swapped(value, "col")])
    return jnp.concatenate(shifts(pairs, "row"))


def piece_places(core, rows):
    peers = lax.axis_size("row")
    piece = np.arange(2 * peers)
    row = lax.rem(lax.axis_index("row") + (peers - piece // 2), peers)
    col = lax.rem(lax.axis_index("col") + piece % 2, 2)
    side = lax.rem(core + np.arange(2), 2)
    return ((row * 2 + col) * rows)[None, :] + (side * (rows // 2))[:, None]


def exchanged(pieces, axis):
    return lax.all_to_all(pieces, axis, 0, 0, tiled=True)


def half_of(value, dim, which):
    size = value.shape[dim] // 2
    return lax.dynamic_slice_in_dim(value, which * size, size, dim)


def pack_kernel(row_ref, factor_ref, theirs_ref, out_ref):
    rows, width = out_ref.shape[2], out_ref.shape[3]
    start = pl.multiple_of(row_ref[0], rows)
    for q in range(out_ref.shape[0]):
        lanes = slice(q * width, (q + 1) * width)
        out_ref[q, 0] = factor_ref[pl.ds(start, rows), lanes]
        out_ref[q, 1] = theirs_ref[:, lanes]


def packed(row, factor, theirs, parts):
    rows, columns = theirs.shape
    vmem = pl.BlockSpec(memory_space=pltpu.VMEM)
    return pl.pallas_call(
        pack_kernel,
        out_shape=jax.ShapeDtypeStruct((parts, 2, rows, columns // parts), factor.dtype),
        in_specs=[pl.BlockSpec(memory_space=pltpu.SMEM), vmem, vmem],
        out_specs=vmem,
        cost_estimate=pl.CostEstimate(flops=1_000_000, bytes_accessed=4 * rows * columns * 2, transcendentals=0),
        name="packed",
    )(row, factor, theirs)


def ordered(first, second, flip):
    return jnp.where(flip == 0, first, second), jnp.where(flip == 0, second, first)


def per_device(border, panel_border, kinv, factor, root_block):
    core = lax.axis_index(CORE)
    scen = lax.axis_index(SCEN)
    col = lax.axis_index("col")
    plane = lax.axis_index(("row", "col"))
    chips = lax.axis_size(CHIPS)
    groups, rows, n = border.shape[1], border.shape[2], border.shape[3]
    width = panel_border.shape[2]

    theirs = swapped(half_of(factor, 0, 1 - col), "col")
    solved = jnp.einsum(
        "snm,smp->snp", kinv, panel_border, preferred_element_type=F32
    ).astype(BF16)
    theirs, solved = lax.optimization_barrier((theirs, solved))
    slices = packed((col * rows).astype(jnp.int32).reshape(1), factor, theirs, chips)
    slices = exchanged(slices, CHIPS)
    coupling = jnp.einsum("sgrn,snp->grp", border, solved, preferred_element_type=F32)
    coupling = coupling.reshape(chips, 2, rows, width)
    slices, coupling = lax.optimization_barrier((slices, coupling))
    bulk = half_of(coupling, 1, core)[:, 0] + swapped(half_of(coupling, 1, 1 - core)[:, 0], CORE)

    keep, send = ordered(slices[0, 0], slices[0, 1], col)
    head = jnp.where(core == 0, keep, lax.ppermute(send, CORE, [(0, 1)]))
    leading = all_planes(head).reshape(-1, head.shape[-1])

    own_solved = lax.dynamic_slice_in_dim(solved, plane * rows, rows, 2)
    panel = jnp.einsum("snr,snp->rp", own_solved, panel_border, preferred_element_type=F32)
    panel = panel + jnp.where(scen == 0, root_block, 0.0)
    panel = panel - lax.dot_general(
        head, leading, (((1,), (1,)), ((), ())), preferred_element_type=F32
    )
    panel = half_of(panel, 0, core) + swapped(half_of(panel, 0, 1 - core), CORE)
    panel = sum(shifts(panel, "scen_1"))
    panel = sum(shifts(panel, "scen_0"))
    own = plane_pieces(panel)
    other = swapped(own, CORE)
    inverse = inverse_factor(piece_places(core, rows), own, other)

    leads = ordered(leading, swapped(leading, CORE), core)
    leads = ordered(*leads, col)
    for slot in range(2):
        bulk = bulk - lax.dot_general(
            slices[:, slot], leads[slot], (((2,), (1,)), ((), ())), preferred_element_type=F32
        )
    pieces = exchanged(bulk.astype(BF16), CHIPS)
    schur = root_block + jnp.sum(pieces.astype(F32), axis=0)
    return lax.dot_general(
        schur, inverse, (((1,), (1,)), ((), ())),
        precision=lax.Precision.HIGHEST, preferred_element_type=F32,
    )


def solution(mesh):
    split = Mesh(
        mesh.devices.reshape(4, 4, 2, mesh.shape["row"], mesh.shape["col"]),
        ("scen_0", "scen_1", "scen_2", "row", "col"),
    )
    in_specs = (
        P(SCEN, None, ("row", "col"), None),
        P(SCEN, None, None),
        P(SCEN, None, None),
        P(SCEN_ROW, "col"),
        P(SCEN_ROW_COL, None),
    )
    out_specs = P(SCEN_ROW_COL, None)
    return jax.shard_map(
        per_device, mesh=split, in_specs=in_specs, out_specs=out_specs, check_vma=False
    )
```

```python
import jax
import jax.numpy as jnp
import numpy as np
from jax import lax
from jax.experimental import pallas as pl
from jax.experimental.pallas import tpu as pltpu
from jax.sharding import Mesh
from jax.sharding import PartitionSpec as P

CHIPS = ("scen_0", "scen_1")
CORE = "scen_2"
SCEN = ("scen_0", "scen_1", "scen_2")
SCEN_ROW = ("scen_0", "scen_1", "scen_2", "row")
SCEN_ROW_COL = ("scen_0", "scen_1", "scen_2", "row", "col")
BF16 = jnp.bfloat16

BLOCK = 128
F32 = jnp.float32


def spread_row(value, row):
    return jnp.broadcast_to(value[row : row + 1, :], value.shape)


def spread_lane(value, lane):
    return jnp.broadcast_to(value[:, lane : lane + 1], value.shape)


def factor_block(rows):
    groups = len(rows)
    tile = rows[0].shape
    sub = lax.broadcasted_iota(jnp.int32, tile, 0)
    lane = lax.broadcasted_iota(jnp.int32, tile, 1)
    inverse = [jnp.where(lane == sub + 8 * g, 1.0, 0.0).astype(F32) for g in range(groups)]
    rows = list(rows)
    done = []
    for t in range(groups):
        cols = [spread_lane(rows[t], 8 * t + j) for j in range(8)]
        left, right = rows[t], inverse[t]
        ahead = inverse[t]
        scale = jnp.zeros(tile, F32)
        square = jnp.zeros(tile, F32)
        for k in range(8):
            root = lax.rsqrt(spread_row(cols[k], k))
            recip = root * root
            scale = jnp.where(sub == k, root, scale)
            square = jnp.where(sub == k, recip, square)
            full = jnp.where(sub == k, 0.0, cols[k] * recip)
            below = jnp.where(sub > k, full, 0.0)
            for j in range(k + 1, 8):
                cols[j] = cols[j] - full * spread_row(cols[j], k)
            left = left - full * spread_row(left, k)
            right = right - full * spread_row(right, k)
            ahead = ahead - below * spread_row(ahead, k)
        done.append(ahead * scale)
        if t == groups - 1:
            break
        left, right = left * square, right * square
        lefts = [spread_row(left, j) for j in range(8)]
        rights = [spread_row(right, j) for j in range(8)]
        for g in range(t + 1, groups):
            coef = [spread_lane(rows[g], 8 * t + j) for j in range(8)]
            a = [coef[j] * lefts[j] for j in range(8)]
            b = [coef[j] * rights[j] for j in range(8)]
            while len(a) > 1:
                a = [a[i] + a[i + 1] for i in range(0, len(a), 2)]
                b = [b[i] + b[i + 1] for i in range(0, len(b), 2)]
            rows[g] = rows[g] - a[0]
            inverse[g] = inverse[g] - b[0]
    return done


def split(value):
    high = value.astype(BF16)
    return high, (value - high.astype(F32)).astype(BF16)


def dot(a, b, dims=((1,), (0,))):
    (ah, al), (bh, bl) = split(a), split(b)
    terms = [
        lax.dot_general(x, y, (dims, ((), ())), preferred_element_type=F32)
        for x, y in ((al, bh), (ah, bl), (ah, bh))
    ]
    return terms[0] + terms[1] + terms[2]


TILES = tuple((i, j) for i in range(4) for j in range(i, 4))


def tile_rows(i, j):
    at = TILES.index((i, j)) * BLOCK
    return slice(at, at + BLOCK)


def inverse_kernel(place_ref, *refs):
    part_refs, (w_ref, s_ref, d_ref) = refs[:-3], refs[-3:]
    n = w_ref.shape[0]
    blocks = n // BLOCK
    count = place_ref.shape[0] // len(part_refs)
    size = part_refs[0].shape[0] // count
    for p, part in enumerate(part_refs):
        for q in range(count):
            at = pl.multiple_of(place_ref[p * count + q], 8)
            s_ref[pl.ds(at, size), :] = part[q * size : (q + 1) * size, :]

    def finish(k):
        lo, hi = k * BLOCK, (k + 1) * BLOCK
        w = d_ref[...]
        if k > 0:
            w_ref[lo:hi, 0:lo] = dot(w, w_ref[lo:hi, 0:lo])
        w_ref[lo:hi, lo:hi] = w
        if hi == n:
            return
        w_ref[lo:hi, hi:n] = jnp.zeros((BLOCK, n - hi), F32)
        u = dot(w, jnp.concatenate([s_ref[tile_rows(k, j), :] for j in range(k + 1, blocks)], axis=1))
        for i in range(k + 1, blocks):
            il, ih = i * BLOCK, (i + 1) * BLOCK
            ui = u[:, il - hi : ih - hi]
            drop = dot(ui, u[:, il - hi :], ((0,), (0,)))
            for j in range(i, blocks):
                cut = (j - i) * BLOCK
                s_ref[tile_rows(i, j), :] = s_ref[tile_rows(i, j), :] - drop[:, cut : cut + BLOCK]
            new = dot(ui, w_ref[lo:hi, 0:hi], ((0,), (0,)))
            if k > 0:
                w_ref[il:ih, 0:lo] = w_ref[il:ih, 0:lo] - new[:, 0:lo]
            w_ref[il:ih, lo:hi] = -new[:, lo:hi]

    def step(k, carry):
        own = (k * blocks - k * (k - 1) // 2) * BLOCK
        done = factor_block(
            [s_ref[pl.ds(pl.multiple_of(own + 8 * g, 8), 8), :] for g in range(BLOCK // 8)]
        )
        for g in range(BLOCK // 8):
            d_ref[8 * g : 8 * g + 8, :] = done[g]
        for static in range(blocks):
            pl.when(k == static)(lambda static=static: finish(static))
        return carry

    lax.fori_loop(0, blocks, step, 0)


def inverse_factor(place, parts, n):
    vmem = pl.BlockSpec(memory_space=pltpu.VMEM)
    return pl.pallas_call(
        inverse_kernel,
        out_shape=jax.ShapeDtypeStruct((n, n), F32),
        in_specs=[pl.BlockSpec(memory_space=pltpu.SMEM)] + [vmem] * len(parts),
        out_specs=vmem,
        scratch_shapes=[
            pltpu.VMEM((len(TILES) * BLOCK, BLOCK), F32),
            pltpu.VMEM((BLOCK, BLOCK), F32),
        ],
        cost_estimate=pl.CostEstimate(flops=40_000_000, bytes_accessed=2 * n * n * 4, transcendentals=n),
        compiler_params=pltpu.CompilerParams(vmem_limit_bytes=12 * 2**20),
        name="inverse_factor",
    )(place, *parts)


def panel_kernel(place_ref, gram_ref, *refs):
    parts = (len(refs) - 4) // 2
    lead_parts, root_parts = refs[:parts], refs[parts : 2 * parts]
    mine_ref, theirs_ref, lead_ref, root_ref = refs[2 * parts :]
    rows = lead_parts[0].shape[1]
    for p in range(parts):
        for q in range(2):
            at = pl.multiple_of(place_ref[2 * p + q], rows)
            lead_ref[pl.ds(at, rows), :] = lead_parts[p][q]
            root_ref[pl.ds(at, rows), :] = root_parts[p][q]
    core = place_ref[2 * parts]
    half = len(TILES) // 2
    for b, (i, j) in enumerate(TILES):
        top, side = slice(i * BLOCK, (i + 1) * BLOCK), slice(j * BLOCK, (j + 1) * BLOCK)
        square = lax.dot_general(
            lead_ref[top, :], lead_ref[side, :], (((1,), (1,)), ((), ())), preferred_element_type=F32
        )
        value = root_ref[top, side] + gram_ref[top, side] - square
        keep = core == b // half
        at = slice(b % half * BLOCK, (b % half + 1) * BLOCK)

        @pl.when(keep)
        def _():
            mine_ref[at, :] = value

        @pl.when(jnp.logical_not(keep))
        def _():
            theirs_ref[at, :] = value


def panel_halves(place, gram, leads, roots):
    vmem = pl.BlockSpec(memory_space=pltpu.VMEM)
    n = gram.shape[0]
    half = jax.ShapeDtypeStruct((len(TILES) // 2 * BLOCK, BLOCK), F32)
    return pl.pallas_call(
        panel_kernel,
        out_shape=(half, half, jax.ShapeDtypeStruct((n, leads[0].shape[-1]), BF16)),
        in_specs=[pl.BlockSpec(memory_space=pltpu.SMEM)] + [vmem] * (1 + len(leads) + len(roots)),
        out_specs=(vmem, vmem, vmem),
        scratch_shapes=[pltpu.VMEM((n, n), F32)],
        cost_estimate=pl.CostEstimate(flops=2_000_000, bytes_accessed=4 * n * n * 4, transcendentals=0),
        compiler_params=pltpu.CompilerParams(vmem_limit_bytes=12 * 2**20),
        name="panel_halves",
    )(place, gram, *leads, *roots)


def coupling_kernel(core_ref, border_ref, solved_ref, sent_ref, kept_ref):
    scens, step, _, rows, n = border_ref.shape
    left = jnp.concatenate([border_ref[s, :, 0].reshape(step * rows, n) for s in range(scens)], axis=1)
    right = solved_ref[...].reshape(scens * n, solved_ref.shape[-1])
    total = jnp.dot(left, right, preferred_element_type=F32).reshape(sent_ref.shape)
    first = pl.program_id(0) < pl.num_programs(0) // 2

    @pl.when(first)
    def _():
        sent_ref[...] = total

    @pl.when(jnp.logical_not(first))
    def _():
        kept_ref[...] = total


def coupling_halves(core, border, solved, step=8):
    scens, chips, _, rows, n = border.shape
    width = solved.shape[-1]
    steps = chips // step
    half = jax.ShapeDtypeStruct((chips, rows, width), F32)
    grid_spec = pltpu.PrefetchScalarGridSpec(
        num_scalar_prefetch=1,
        grid=(2 * steps,),
        in_specs=[
            pl.BlockSpec(
                (scens, step, 1, rows, n),
                lambda t, c: (0, lax.rem(t, steps), lax.rem(c[0] + 1 + t // steps, 2), 0, 0),
            ),
            pl.BlockSpec((scens, n, width), lambda t, c: (0, 0, 0)),
        ],
        out_specs=[
            pl.BlockSpec((step, rows, width), lambda t, c: (jnp.minimum(t, steps - 1), 0, 0)),
            pl.BlockSpec((step, rows, width), lambda t, c: (jnp.maximum(t - steps, 0), 0, 0)),
        ],
    )
    return pl.pallas_call(
        coupling_kernel,
        out_shape=(half, half),
        grid_spec=grid_spec,
        compiler_params=pltpu.CompilerParams(dimension_semantics=("arbitrary",)),
        cost_estimate=pl.CostEstimate(
            flops=4 * scens * chips * rows * n * width,
            bytes_accessed=2 * scens * chips * rows * n * 2 + 2 * chips * rows * width * 4,
            transcendentals=0,
        ),
        name="coupling_halves",
    )(core, border, solved)


def swapped(value, axis):
    return lax.ppermute(value, axis, [(0, 1), (1, 0)])


def shifts(value, axis):
    peers = lax.axis_size(axis)
    return [value] + [
        lax.ppermute(value, axis, [(i, (i + step) % peers) for i in range(peers)])
        for step in range(1, peers)
    ]


def plane_parts(value):
    return shifts(jnp.stack([value, swapped(value, "col")]), "row")


def plane_parts_of_first(value):
    rows = lax.axis_size("row")
    pairs = jnp.stack([value, lax.ppermute(value, (*SCEN, "col"), [(0, 1), (1, 0)])])
    return [pairs] + [
        lax.ppermute(pairs, (*SCEN, "row"), [(i, (i + step) % rows) for i in range(rows)])
        for step in range(1, rows)
    ]


def part_places(rows):
    peers = lax.axis_size("row")
    part = np.arange(2 * peers)
    row = lax.rem(lax.axis_index("row") + (peers - part // 2), peers)
    col = lax.rem(lax.axis_index("col") + part % 2, 2)
    return (row * 2 + col) * rows


def piece_places(core, size):
    across, down = lax.axis_size("scen_1"), lax.axis_size("scen_0")
    piece = np.arange(2 * across * down)
    side = lax.rem(core + piece // (across * down), 2)
    x = lax.rem(lax.axis_index("scen_1") + (across - piece // down % across), across)
    y = lax.rem(lax.axis_index("scen_0") + (down - piece % down), down)
    return ((side * across + x) * down + y) * size


def scattered_sum(value, axis):
    peers = lax.axis_size(axis)
    place = lax.axis_index(axis)
    size = value.shape[0] // peers
    total = lax.dynamic_slice_in_dim(value, place * size, size, 0)
    for step in range(1, peers):
        piece = lax.dynamic_slice_in_dim(value, lax.rem(place + step, peers) * size, size, 0)
        total = total + lax.ppermute(piece, axis, [(i, (i + step) % peers) for i in range(peers)])
    return total


def exchanged(pieces, axis):
    return lax.all_to_all(pieces, axis, 0, 0, tiled=True)


def half_of(value, dim, which):
    size = value.shape[dim] // 2
    return lax.dynamic_slice_in_dim(value, which * size, size, dim)


def pack_kernel(row_ref, factor_ref, theirs_ref, out_ref):
    rows, width = out_ref.shape[2], out_ref.shape[3]
    start = pl.multiple_of(row_ref[0], rows)
    for q in range(out_ref.shape[0]):
        lanes = slice(q * width, (q + 1) * width)
        out_ref[q, 0] = factor_ref[pl.ds(start, rows), lanes]
        out_ref[q, 1] = theirs_ref[:, lanes]


def packed(row, factor, theirs, parts):
    rows, columns = theirs.shape
    vmem = pl.BlockSpec(memory_space=pltpu.VMEM)
    return pl.pallas_call(
        pack_kernel,
        out_shape=jax.ShapeDtypeStruct((parts, 2, rows, columns // parts), factor.dtype),
        in_specs=[pl.BlockSpec(memory_space=pltpu.SMEM), vmem, vmem],
        out_specs=vmem,
        cost_estimate=pl.CostEstimate(flops=1_000_000, bytes_accessed=4 * rows * columns * 2, transcendentals=0),
        compiler_params=pltpu.CompilerParams(vmem_limit_bytes=12 * 2**20),
        name="packed",
    )(row, factor, theirs)


def ordered(first, second, flip):
    return jnp.where(flip == 0, first, second), jnp.where(flip == 0, second, first)


def per_device(border, panel_border, kinv, factor, root_block):
    core = lax.axis_index(CORE).astype(jnp.int32)
    scen = lax.axis_index(SCEN)
    col = lax.axis_index("col")
    chips = lax.axis_size(CHIPS)
    rows = border.shape[2]
    width = panel_border.shape[2]

    theirs = swapped(half_of(factor, 0, 1 - col), "col")
    roots = plane_parts_of_first(jnp.where(scen == 0, root_block, 0.0))
    solved = jnp.einsum(
        "snm,smp->snp", kinv, panel_border, preferred_element_type=F32
    ).astype(BF16)
    theirs, solved = lax.optimization_barrier((theirs, solved))
    slices = packed((col * rows).astype(jnp.int32).reshape(1), factor, theirs, chips)
    slices = exchanged(slices, CHIPS)
    halves = border.reshape(border.shape[0], chips, 2, rows, border.shape[3])
    sent, kept = coupling_halves(core.reshape(1), halves, solved)
    gram = jnp.einsum("snr,snp->rp", solved, panel_border, preferred_element_type=F32)
    slices, sent, kept, gram, roots = lax.optimization_barrier((slices, sent, kept, gram, roots))
    bulk = kept + swapped(sent, CORE)

    keep, send = ordered(slices[0, 0], slices[0, 1], col)
    head = jnp.where(core == 0, keep, lax.ppermute(send, CORE, [(0, 1)]))
    place = jnp.concatenate([part_places(rows).astype(jnp.int32), core.reshape(1)])
    mine, theirs, leading = panel_halves(place, gram, plane_parts(head), roots)
    piece = mine + swapped(theirs, CORE)
    piece = scattered_sum(piece, "scen_1")
    piece = scattered_sum(piece, "scen_0")
    place = piece_places(core, piece.shape[0]).astype(jnp.int32)
    own = shifts(jnp.concatenate(shifts(piece, "scen_0")), "scen_1")
    inverse = inverse_factor(place, own + [swapped(part, CORE) for part in own], width)

    leads = ordered(leading, swapped(leading, CORE), core)
    leads = ordered(*leads, col)
    for slot in range(2):
        bulk = bulk - lax.dot_general(
            slices[:, slot], leads[slot], (((2,), (1,)), ((), ())), preferred_element_type=F32
        )
    pieces = exchanged(bulk.astype(BF16), CHIPS)
    schur = root_block + jnp.sum(pieces.astype(F32), axis=0)
    return lax.dot_general(
        schur, inverse, (((1,), (1,)), ((), ())),
        precision=lax.Precision.HIGH, preferred_element_type=F32,
    )


def solution(mesh):
    split = Mesh(
        mesh.devices.reshape(4, 4, 2, mesh.shape["row"], mesh.shape["col"]),
        ("scen_0", "scen_1", "scen_2", "row", "col"),
    )
    in_specs = (
        P(SCEN, None, ("row", "col"), None),
        P(SCEN, None, None),
        P(SCEN, None, None),
        P(SCEN_ROW, "col"),
        P(SCEN_ROW_COL, None),
    )
    out_specs = P(SCEN_ROW_COL, None)
    return jax.shard_map(
        per_device, mesh=split, in_specs=in_specs, out_specs=out_specs, check_vma=False
    )
```

```python
import jax
import jax.numpy as jnp
import numpy as np
from jax import lax
from jax.experimental import pallas as pl
from jax.experimental.pallas import tpu as pltpu
from jax.sharding import Mesh
from jax.sharding import PartitionSpec as P

CHIPS = ("scen_0", "scen_1")
CORE = "scen_2"
SCEN = ("scen_0", "scen_1", "scen_2")
SCEN_ROW = ("scen_0", "scen_1", "scen_2", "row")
SCEN_ROW_COL = ("scen_0", "scen_1", "scen_2", "row", "col")
BF16 = jnp.bfloat16

BLOCK = 128
F32 = jnp.float32


def spread_row(value, row):
    return jnp.broadcast_to(value[row : row + 1, :], value.shape)


def spread_lane(value, lane):
    return jnp.broadcast_to(value[:, lane : lane + 1], value.shape)


def factor_block(rows):
    groups = len(rows)
    tile = rows[0].shape
    sub = lax.broadcasted_iota(jnp.int32, tile, 0)
    lane = lax.broadcasted_iota(jnp.int32, tile, 1)
    inverse = [jnp.where(lane == sub + 8 * g, 1.0, 0.0).astype(F32) for g in range(groups)]
    rows = list(rows)
    done = []
    for t in range(groups):
        cols = [spread_lane(rows[t], 8 * t + j) for j in range(8)]
        left, right = rows[t], inverse[t]
        ahead = inverse[t]
        scale = jnp.zeros(tile, F32)
        square = jnp.zeros(tile, F32)
        for k in range(8):
            root = lax.rsqrt(spread_row(cols[k], k))
            recip = root * root
            scale = jnp.where(sub == k, root, scale)
            square = jnp.where(sub == k, recip, square)
            full = jnp.where(sub == k, 0.0, cols[k] * recip)
            below = jnp.where(sub > k, full, 0.0)
            for j in range(k + 1, 8):
                cols[j] = cols[j] - full * spread_row(cols[j], k)
            left = left - full * spread_row(left, k)
            right = right - full * spread_row(right, k)
            ahead = ahead - below * spread_row(ahead, k)
        done.append(ahead * scale)
        if t == groups - 1:
            break
        left, right = left * square, right * square
        lefts = [spread_row(left, j) for j in range(8)]
        rights = [spread_row(right, j) for j in range(8)]
        for g in range(t + 1, groups):
            coef = [spread_lane(rows[g], 8 * t + j) for j in range(8)]
            a = [coef[j] * lefts[j] for j in range(8)]
            b = [coef[j] * rights[j] for j in range(8)]
            while len(a) > 1:
                a = [a[i] + a[i + 1] for i in range(0, len(a), 2)]
                b = [b[i] + b[i + 1] for i in range(0, len(b), 2)]
            rows[g] = rows[g] - a[0]
            inverse[g] = inverse[g] - b[0]
    return done


def split(value):
    high = value.astype(BF16)
    return high, (value - high.astype(F32)).astype(BF16)


def dot(a, b, dims=((1,), (0,))):
    (ah, al), (bh, bl) = split(a), split(b)
    terms = [
        lax.dot_general(x, y, (dims, ((), ())), preferred_element_type=F32)
        for x, y in ((al, bh), (ah, bl), (ah, bh))
    ]
    return terms[0] + terms[1] + terms[2]


def inverse_kernel(place_ref, *refs):
    part_refs, (w_ref, s_ref, d_ref) = refs[:-3], refs[-3:]
    n = w_ref.shape[0]
    blocks = n // BLOCK
    count, size, _ = part_refs[0].shape
    for p, part in enumerate(part_refs):
        for q in range(count):
            at = pl.multiple_of(place_ref[p * count + q], size)
            s_ref[pl.ds(at, size), :] = part[q]

    def finish(k):
        lo, hi = k * BLOCK, (k + 1) * BLOCK
        w = d_ref[...]
        if k > 0:
            w_ref[lo:hi, 0:lo] = dot(w, w_ref[lo:hi, 0:lo])
        w_ref[lo:hi, lo:hi] = w
        if hi == n:
            return
        w_ref[lo:hi, hi:n] = jnp.zeros((BLOCK, n - hi), F32)
        u = dot(w, s_ref[lo:hi, hi:n])
        for i in range(k + 1, blocks):
            il, ih = i * BLOCK, (i + 1) * BLOCK
            ui = u[:, il - hi : ih - hi]
            s_ref[il:ih, il:n] = s_ref[il:ih, il:n] - dot(ui, u[:, il - hi :], ((0,), (0,)))
            new = dot(ui, w_ref[lo:hi, 0:hi], ((0,), (0,)))
            if k > 0:
                w_ref[il:ih, 0:lo] = w_ref[il:ih, 0:lo] - new[:, 0:lo]
            w_ref[il:ih, lo:hi] = -new[:, lo:hi]

    def step(k, carry):
        lanes = pl.ds(pl.multiple_of(k * BLOCK, BLOCK), BLOCK)
        done = factor_block(
            [s_ref[pl.ds(pl.multiple_of(k * BLOCK + 8 * g, 8), 8), lanes] for g in range(BLOCK // 8)]
        )
        for g in range(BLOCK // 8):
            d_ref[8 * g : 8 * g + 8, :] = done[g]
        for static in range(blocks):
            pl.when(k == static)(lambda static=static: finish(static))
        return carry

    lax.fori_loop(0, blocks, step, 0)


def inverse_factor(place, parts):
    vmem = pl.BlockSpec(memory_space=pltpu.VMEM)
    n = parts[0].shape[-1]
    return pl.pallas_call(
        inverse_kernel,
        out_shape=jax.ShapeDtypeStruct((n, n), F32),
        in_specs=[pl.BlockSpec(memory_space=pltpu.SMEM)] + [vmem] * len(parts),
        out_specs=vmem,
        scratch_shapes=[pltpu.VMEM((n, n), F32), pltpu.VMEM((BLOCK, BLOCK), F32)],
        cost_estimate=pl.CostEstimate(flops=40_000_000, bytes_accessed=2 * n * n * 4, transcendentals=n),
        compiler_params=pltpu.CompilerParams(vmem_limit_bytes=12 * 2**20),
        name="inverse_factor",
    )(place, *parts)


def panel_kernel(place_ref, head_ref, base_ref, *refs):
    lead_parts, (mine_ref, theirs_ref, lead_ref, rows_ref) = refs[:-4], refs[-4:]
    rows = head_ref.shape[0]
    for p, part in enumerate(lead_parts):
        for q in range(2):
            at = pl.multiple_of(place_ref[2 * p + q], rows)
            lead_ref[pl.ds(at, rows), :] = part[q]
    rows_ref[...] = base_ref[...] - lax.dot_general(
        head_ref[...], lead_ref[...], (((1,), (1,)), ((), ())), preferred_element_type=F32
    )
    half = rows // 2
    own = pl.multiple_of(place_ref[2 * len(lead_parts)], half)
    mine_ref[...] = rows_ref[pl.ds(own, half), :]
    theirs_ref[...] = rows_ref[pl.ds(pl.multiple_of(half - own, half), half), :]


def panel_rows(place, head, base, leads):
    vmem = pl.BlockSpec(memory_space=pltpu.VMEM)
    rows, n = base.shape
    half = jax.ShapeDtypeStruct((rows // 2, n), F32)
    return pl.pallas_call(
        panel_kernel,
        out_shape=(half, half, jax.ShapeDtypeStruct((n, head.shape[-1]), BF16)),
        in_specs=[pl.BlockSpec(memory_space=pltpu.SMEM)] + [vmem] * (2 + len(leads)),
        out_specs=(vmem, vmem, vmem),
        scratch_shapes=[pltpu.VMEM((rows, n), F32)],
        cost_estimate=pl.CostEstimate(flops=1_000_000, bytes_accessed=4 * rows * n * 4, transcendentals=0),
        compiler_params=pltpu.CompilerParams(vmem_limit_bytes=12 * 2**20),
        name="panel_rows",
    )(place, head, base, *leads)


def coupling_kernel(core_ref, border_ref, solved_ref, sent_ref, kept_ref):
    scens, step, _, rows, n = border_ref.shape
    left = jnp.concatenate([border_ref[s, :, 0].reshape(step * rows, n) for s in range(scens)], axis=1)
    right = solved_ref[...].reshape(scens * n, solved_ref.shape[-1])
    total = jnp.dot(left, right, preferred_element_type=F32).reshape(sent_ref.shape)
    first = pl.program_id(0) < pl.num_programs(0) // 2

    @pl.when(first)
    def _():
        sent_ref[...] = total

    @pl.when(jnp.logical_not(first))
    def _():
        kept_ref[...] = total


def coupling_halves(core, border, solved, step=8):
    scens, chips, _, rows, n = border.shape
    width = solved.shape[-1]
    steps = chips // step
    half = jax.ShapeDtypeStruct((chips, rows, width), F32)
    grid_spec = pltpu.PrefetchScalarGridSpec(
        num_scalar_prefetch=1,
        grid=(2 * steps,),
        in_specs=[
            pl.BlockSpec(
                (scens, step, 1, rows, n),
                lambda t, c: (0, lax.rem(t, steps), lax.rem(c[0] + 1 + t // steps, 2), 0, 0),
            ),
            pl.BlockSpec((scens, n, width), lambda t, c: (0, 0, 0)),
        ],
        out_specs=[
            pl.BlockSpec((step, rows, width), lambda t, c: (jnp.minimum(t, steps - 1), 0, 0)),
            pl.BlockSpec((step, rows, width), lambda t, c: (jnp.maximum(t - steps, 0), 0, 0)),
        ],
    )
    return pl.pallas_call(
        coupling_kernel,
        out_shape=(half, half),
        grid_spec=grid_spec,
        compiler_params=pltpu.CompilerParams(dimension_semantics=("arbitrary",)),
        cost_estimate=pl.CostEstimate(
            flops=4 * scens * chips * rows * n * width,
            bytes_accessed=2 * scens * chips * rows * n * 2 + 2 * chips * rows * width * 4,
            transcendentals=0,
        ),
        name="coupling_halves",
    )(core, border, solved)


def swapped(value, axis):
    return lax.ppermute(value, axis, [(0, 1), (1, 0)])


def shifts(value, axis):
    peers = lax.axis_size(axis)
    return [value] + [
        lax.ppermute(value, axis, [(i, (i + step) % peers) for i in range(peers)])
        for step in range(1, peers)
    ]


def plane_parts(value):
    pairs = jnp.stack([value, swapped(value, "col")])
    return shifts(pairs, "row")


def part_places(rows):
    peers = lax.axis_size("row")
    part = np.arange(2 * peers)
    row = lax.rem(lax.axis_index("row") + (peers - part // 2), peers)
    col = lax.rem(lax.axis_index("col") + part % 2, 2)
    return (row * 2 + col) * rows


def exchanged(pieces, axis):
    return lax.all_to_all(pieces, axis, 0, 0, tiled=True)


def half_of(value, dim, which):
    size = value.shape[dim] // 2
    return lax.dynamic_slice_in_dim(value, which * size, size, dim)


def pack_kernel(row_ref, factor_ref, theirs_ref, out_ref):
    rows, width = out_ref.shape[2], out_ref.shape[3]
    start = pl.multiple_of(row_ref[0], rows)
    for q in range(out_ref.shape[0]):
        lanes = slice(q * width, (q + 1) * width)
        out_ref[q, 0] = factor_ref[pl.ds(start, rows), lanes]
        out_ref[q, 1] = theirs_ref[:, lanes]


def packed(row, factor, theirs, parts):
    rows, columns = theirs.shape
    vmem = pl.BlockSpec(memory_space=pltpu.VMEM)
    return pl.pallas_call(
        pack_kernel,
        out_shape=jax.ShapeDtypeStruct((parts, 2, rows, columns // parts), factor.dtype),
        in_specs=[pl.BlockSpec(memory_space=pltpu.SMEM), vmem, vmem],
        out_specs=vmem,
        cost_estimate=pl.CostEstimate(flops=1_000_000, bytes_accessed=4 * rows * columns * 2, transcendentals=0),
        compiler_params=pltpu.CompilerParams(vmem_limit_bytes=12 * 2**20),
        name="packed",
    )(row, factor, theirs)


def ordered(first, second, flip):
    return jnp.where(flip == 0, first, second), jnp.where(flip == 0, second, first)


def per_device(border, panel_border, kinv, factor, root_block):
    core = lax.axis_index(CORE).astype(jnp.int32)
    scen = lax.axis_index(SCEN)
    col = lax.axis_index("col")
    chips = lax.axis_size(CHIPS)
    rows = border.shape[2]
    plane = lax.axis_index(("row", "col"))

    theirs = swapped(half_of(factor, 0, 1 - col), "col")
    solved = jnp.einsum(
        "snm,smp->snp", kinv, panel_border, preferred_element_type=F32
    ).astype(BF16)
    theirs, solved = lax.optimization_barrier((theirs, solved))
    slices = packed((col * rows).astype(jnp.int32).reshape(1), factor, theirs, chips)
    slices = exchanged(slices, CHIPS)
    halves = border.reshape(border.shape[0], chips, 2, rows, border.shape[3])
    sent, kept = coupling_halves(core.reshape(1), halves, solved)
    slices, sent, kept = lax.optimization_barrier((slices, sent, kept))
    bulk = kept + swapped(sent, CORE)

    keep, send = ordered(slices[0, 0], slices[0, 1], col)
    head = jnp.where(core == 0, keep, lax.ppermute(send, CORE, [(0, 1)]))
    own_solved = lax.dynamic_slice_in_dim(solved, plane * rows, rows, 2)
    base = jnp.einsum("snr,snp->rp", own_solved, panel_border, preferred_element_type=F32)
    base = base + jnp.where(scen == 0, root_block, 0.0)
    places = part_places(rows).astype(jnp.int32)
    offset = core.reshape(1) * (rows // 2)
    mine, theirs, leading = panel_rows(
        jnp.concatenate([places, offset]), head, base, plane_parts(head)
    )
    panel = mine + swapped(theirs, CORE)
    panel = sum(shifts(panel, "scen_1"))
    panel = sum(shifts(panel, "scen_0"))
    own = plane_parts(panel)
    places = jnp.concatenate([places + offset, places + (rows // 2 - offset)])
    inverse = inverse_factor(places, own + [swapped(part, CORE) for part in own])

    leads = ordered(leading, swapped(leading, CORE), core)
    leads = ordered(*leads, col)
    for slot in range(2):
        bulk = bulk - lax.dot_general(
            slices[:, slot], leads[slot], (((2,), (1,)), ((), ())), preferred_element_type=F32
        )
    pieces = exchanged(bulk.astype(BF16), CHIPS)
    schur = root_block + jnp.sum(pieces.astype(F32), axis=0)
    return lax.dot_general(
        schur, inverse, (((1,), (1,)), ((), ())),
        precision=lax.Precision.HIGH, preferred_element_type=F32,
    )


def solution(mesh):
    split = Mesh(
        mesh.devices.reshape(4, 4, 2, mesh.shape["row"], mesh.shape["col"]),
        ("scen_0", "scen_1", "scen_2", "row", "col"),
    )
    in_specs = (
        P(SCEN, None, ("row", "col"), None),
        P(SCEN, None, None),
        P(SCEN, None, None),
        P(SCEN_ROW, "col"),
        P(SCEN_ROW_COL, None),
    )
    out_specs = P(SCEN_ROW_COL, None)
    return jax.shard_map(
        per_device, mesh=split, in_specs=in_specs, out_specs=out_specs, check_vma=False
    )
```

```python
import jax
import jax.numpy as jnp
import numpy as np
from jax import lax
from jax.experimental import pallas as pl
from jax.experimental.pallas import tpu as pltpu
from jax.sharding import Mesh
from jax.sharding import PartitionSpec as P

CHIPS = ("scen_0", "scen_1")
CORE = "scen_2"
SCEN = ("scen_0", "scen_1", "scen_2")
SCEN_ROW = ("scen_0", "scen_1", "scen_2", "row")
SCEN_ROW_COL = ("scen_0", "scen_1", "scen_2", "row", "col")
BF16 = jnp.bfloat16

BLOCK = 128
F32 = jnp.float32


def spread_row(value, row):
    return jnp.broadcast_to(value[row : row + 1, :], value.shape)


def spread_lane(value, lane):
    return jnp.broadcast_to(value[:, lane : lane + 1], value.shape)


def factor_block(rows):
    groups = len(rows)
    tile = rows[0].shape
    sub = lax.broadcasted_iota(jnp.int32, tile, 0)
    lane = lax.broadcasted_iota(jnp.int32, tile, 1)
    inverse = [jnp.where(lane == sub + 8 * g, 1.0, 0.0).astype(F32) for g in range(groups)]
    rows = list(rows)
    done = []
    cols = [spread_lane(rows[0], j) for j in range(8)]
    for t in range(groups):
        more = t + 1 < groups
        if more:
            extra = [spread_lane(rows[t], 8 * (t + 1) + j) for j in range(8)]
            following = [spread_lane(rows[t + 1], 8 * (t + 1) + j) for j in range(8)]
        left, right = rows[t], inverse[t]
        ahead = inverse[t]
        scale = jnp.zeros(tile, F32)
        square = jnp.zeros(tile, F32)
        for k in range(8):
            root = lax.rsqrt(spread_row(cols[k], k))
            recip = root * root
            scale = jnp.where(sub == k, root, scale)
            square = jnp.where(sub == k, recip, square)
            full = jnp.where(sub == k, 0.0, cols[k] * recip)
            below = jnp.where(sub > k, full, 0.0)
            for j in range(k + 1, 8):
                cols[j] = cols[j] - full * spread_row(cols[j], k)
            if more:
                extra = [e - full * spread_row(e, k) for e in extra]
            left = left - full * spread_row(left, k)
            right = right - full * spread_row(right, k)
            ahead = ahead - below * spread_row(ahead, k)
        done.append(ahead * scale)
        if t == groups - 1:
            break
        left, right = left * square, right * square
        lefts = [spread_row(left, j) for j in range(8)]
        rights = [spread_row(right, j) for j in range(8)]
        for g in range(t + 1, groups):
            coef = [spread_lane(rows[g], 8 * t + j) for j in range(8)]
            if g == t + 1:
                cols = []
                for j in range(8):
                    scaled = extra[j] * square
                    terms = [coef[m] * spread_row(scaled, m) for m in range(8)]
                    while len(terms) > 1:
                        terms = [terms[i] + terms[i + 1] for i in range(0, len(terms), 2)]
                    cols.append(following[j] - terms[0])
            a = [coef[j] * lefts[j] for j in range(8)]
            b = [coef[j] * rights[j] for j in range(8)]
            while len(a) > 1:
                a = [a[i] + a[i + 1] for i in range(0, len(a), 2)]
                b = [b[i] + b[i + 1] for i in range(0, len(b), 2)]
            rows[g] = rows[g] - a[0]
            inverse[g] = inverse[g] - b[0]
    return done


def split(value):
    high = value.astype(BF16)
    return high, (value - high.astype(F32)).astype(BF16)


def dot(a, b, dims=((1,), (0,))):
    (ah, al), (bh, bl) = split(a), split(b)
    terms = [
        lax.dot_general(x, y, (dims, ((), ())), preferred_element_type=F32)
        for x, y in ((al, bh), (ah, bl), (ah, bh))
    ]
    return terms[0] + terms[1] + terms[2]


def inverse_kernel(place_ref, *refs):
    part_refs, (w_ref, s_ref, d_ref) = refs[:-3], refs[-3:]
    n = w_ref.shape[0]
    blocks = n // BLOCK
    count, size, _ = part_refs[0].shape
    for p, part in enumerate(part_refs):
        for q in range(count):
            at = pl.multiple_of(place_ref[p * count + q], size)
            s_ref[pl.ds(at, size), :] = part[q]

    def finish(k):
        lo, hi = k * BLOCK, (k + 1) * BLOCK
        w = d_ref[...]
        if k > 0:
            w_ref[lo:hi, 0:lo] = dot(w, w_ref[lo:hi, 0:lo])
        w_ref[lo:hi, lo:hi] = w
        if hi == n:
            return
        w_ref[lo:hi, hi:n] = jnp.zeros((BLOCK, n - hi), F32)
        u = dot(w, s_ref[lo:hi, hi:n])
        for i in range(k + 1, blocks):
            il, ih = i * BLOCK, (i + 1) * BLOCK
            ui = u[:, il - hi : ih - hi]
            s_ref[il:ih, il:n] = s_ref[il:ih, il:n] - dot(ui, u[:, il - hi :], ((0,), (0,)))
            new = dot(ui, w_ref[lo:hi, 0:hi], ((0,), (0,)))
            if k > 0:
                w_ref[il:ih, 0:lo] = w_ref[il:ih, 0:lo] - new[:, 0:lo]
            w_ref[il:ih, lo:hi] = -new[:, lo:hi]

    def step(k, carry):
        lanes = pl.ds(pl.multiple_of(k * BLOCK, BLOCK), BLOCK)
        done = factor_block(
            [s_ref[pl.ds(pl.multiple_of(k * BLOCK + 8 * g, 8), 8), lanes] for g in range(BLOCK // 8)]
        )
        for g in range(BLOCK // 8):
            d_ref[8 * g : 8 * g + 8, :] = done[g]
        for static in range(blocks):
            pl.when(k == static)(lambda static=static: finish(static))
        return carry

    lax.fori_loop(0, blocks, step, 0)


def inverse_factor(place, parts):
    vmem = pl.BlockSpec(memory_space=pltpu.VMEM)
    n = parts[0].shape[-1]
    return pl.pallas_call(
        inverse_kernel,
        out_shape=jax.ShapeDtypeStruct((n, n), F32),
        in_specs=[pl.BlockSpec(memory_space=pltpu.SMEM)] + [vmem] * len(parts),
        out_specs=vmem,
        scratch_shapes=[pltpu.VMEM((n, n), F32), pltpu.VMEM((BLOCK, BLOCK), F32)],
        cost_estimate=pl.CostEstimate(flops=40_000_000, bytes_accessed=2 * n * n * 4, transcendentals=n),
        compiler_params=pltpu.CompilerParams(vmem_limit_bytes=12 * 2**20),
        name="inverse_factor",
    )(place, *parts)


def panel_kernel(place_ref, head_ref, base_ref, *refs):
    lead_parts, (mine_ref, theirs_ref, lead_ref, rows_ref) = refs[:-4], refs[-4:]
    rows = head_ref.shape[0]
    for p, part in enumerate(lead_parts):
        for q in range(2):
            at = pl.multiple_of(place_ref[2 * p + q], rows)
            lead_ref[pl.ds(at, rows), :] = part[q]
    rows_ref[...] = base_ref[...] - lax.dot_general(
        head_ref[...], lead_ref[...], (((1,), (1,)), ((), ())), preferred_element_type=F32
    )
    half = rows // 2
    own = pl.multiple_of(place_ref[2 * len(lead_parts)], half)
    mine_ref[...] = rows_ref[pl.ds(own, half), :]
    theirs_ref[...] = rows_ref[pl.ds(pl.multiple_of(half - own, half), half), :]


def panel_rows(place, head, base, leads):
    vmem = pl.BlockSpec(memory_space=pltpu.VMEM)
    rows, n = base.shape
    half = jax.ShapeDtypeStruct((rows // 2, n), F32)
    return pl.pallas_call(
        panel_kernel,
        out_shape=(half, half, jax.ShapeDtypeStruct((n, head.shape[-1]), BF16)),
        in_specs=[pl.BlockSpec(memory_space=pltpu.SMEM)] + [vmem] * (2 + len(leads)),
        out_specs=(vmem, vmem, vmem),
        scratch_shapes=[pltpu.VMEM((rows, n), F32)],
        cost_estimate=pl.CostEstimate(flops=1_000_000, bytes_accessed=4 * rows * n * 4, transcendentals=0),
        compiler_params=pltpu.CompilerParams(vmem_limit_bytes=12 * 2**20),
        name="panel_rows",
    )(place, head, base, *leads)


def coupling_kernel(core_ref, border_ref, solved_ref, sent_ref, kept_ref):
    scens, step, _, rows, n = border_ref.shape
    left = jnp.concatenate([border_ref[s, :, 0].reshape(step * rows, n) for s in range(scens)], axis=1)
    right = solved_ref[...].reshape(scens * n, solved_ref.shape[-1])
    total = jnp.dot(left, right, preferred_element_type=F32).reshape(sent_ref.shape)
    first = pl.program_id(0) < pl.num_programs(0) // 2

    @pl.when(first)
    def _():
        sent_ref[...] = total

    @pl.when(jnp.logical_not(first))
    def _():
        kept_ref[...] = total


def coupling_halves(core, border, solved, step=8):
    scens, chips, _, rows, n = border.shape
    width = solved.shape[-1]
    steps = chips // step
    half = jax.ShapeDtypeStruct((chips, rows, width), F32)
    grid_spec = pltpu.PrefetchScalarGridSpec(
        num_scalar_prefetch=1,
        grid=(2 * steps,),
        in_specs=[
            pl.BlockSpec(
                (scens, step, 1, rows, n),
                lambda t, c: (0, lax.rem(t, steps), lax.rem(c[0] + 1 + t // steps, 2), 0, 0),
            ),
            pl.BlockSpec((scens, n, width), lambda t, c: (0, 0, 0)),
        ],
        out_specs=[
            pl.BlockSpec((step, rows, width), lambda t, c: (jnp.minimum(t, steps - 1), 0, 0)),
            pl.BlockSpec((step, rows, width), lambda t, c: (jnp.maximum(t - steps, 0), 0, 0)),
        ],
    )
    return pl.pallas_call(
        coupling_kernel,
        out_shape=(half, half),
        grid_spec=grid_spec,
        compiler_params=pltpu.CompilerParams(dimension_semantics=("arbitrary",)),
        cost_estimate=pl.CostEstimate(
            flops=4 * scens * chips * rows * n * width,
            bytes_accessed=2 * scens * chips * rows * n * 2 + 2 * chips * rows * width * 4,
            transcendentals=0,
        ),
        name="coupling_halves",
    )(core, border, solved)


def swapped(value, axis):
    return lax.ppermute(value, axis, [(0, 1), (1, 0)])


def shifts(value, axis):
    peers = lax.axis_size(axis)
    return [value] + [
        lax.ppermute(value, axis, [(i, (i + step) % peers) for i in range(peers)])
        for step in range(1, peers)
    ]


def plane_parts(value):
    pairs = jnp.stack([value, swapped(value, "col")])
    return shifts(pairs, "row")


def part_places(rows):
    peers = lax.axis_size("row")
    part = np.arange(2 * peers)
    row = lax.rem(lax.axis_index("row") + (peers - part // 2), peers)
    col = lax.rem(lax.axis_index("col") + part % 2, 2)
    return (row * 2 + col) * rows


def exchanged(pieces, axis):
    return lax.all_to_all(pieces, axis, 0, 0, tiled=True)


def half_of(value, dim, which):
    size = value.shape[dim] // 2
    return lax.dynamic_slice_in_dim(value, which * size, size, dim)


def pack_kernel(row_ref, factor_ref, theirs_ref, out_ref):
    rows, width = out_ref.shape[2], out_ref.shape[3]
    start = pl.multiple_of(row_ref[0], rows)
    for q in range(out_ref.shape[0]):
        lanes = slice(q * width, (q + 1) * width)
        out_ref[q, 0] = factor_ref[pl.ds(start, rows), lanes]
        out_ref[q, 1] = theirs_ref[:, lanes]


def packed(row, factor, theirs, parts):
    rows, columns = theirs.shape
    vmem = pl.BlockSpec(memory_space=pltpu.VMEM)
    return pl.pallas_call(
        pack_kernel,
        out_shape=jax.ShapeDtypeStruct((parts, 2, rows, columns // parts), factor.dtype),
        in_specs=[pl.BlockSpec(memory_space=pltpu.SMEM), vmem, vmem],
        out_specs=vmem,
        cost_estimate=pl.CostEstimate(flops=1_000_000, bytes_accessed=4 * rows * columns * 2, transcendentals=0),
        compiler_params=pltpu.CompilerParams(vmem_limit_bytes=12 * 2**20),
        name="packed",
    )(row, factor, theirs)


def ordered(first, second, flip):
    return jnp.where(flip == 0, first, second), jnp.where(flip == 0, second, first)


def per_device(border, panel_border, kinv, factor, root_block):
    core = lax.axis_index(CORE).astype(jnp.int32)
    scen = lax.axis_index(SCEN)
    col = lax.axis_index("col")
    chips = lax.axis_size(CHIPS)
    rows = border.shape[2]
    plane = lax.axis_index(("row", "col"))

    theirs = swapped(half_of(factor, 0, 1 - col), "col")
    solved = jnp.einsum(
        "snm,smp->snp", kinv, panel_border, preferred_element_type=F32
    ).astype(BF16)
    theirs, solved = lax.optimization_barrier((theirs, solved))
    slices = packed((col * rows).astype(jnp.int32).reshape(1), factor, theirs, chips)
    slices = exchanged(slices, CHIPS)
    halves = border.reshape(border.shape[0], chips, 2, rows, border.shape[3])
    sent, kept = coupling_halves(core.reshape(1), halves, solved)
    slices, sent, kept = lax.optimization_barrier((slices, sent, kept))
    bulk = kept + swapped(sent, CORE)

    keep, send = ordered(slices[0, 0], slices[0, 1], col)
    head = jnp.where(core == 0, keep, lax.ppermute(send, CORE, [(0, 1)]))
    own_solved = lax.dynamic_slice_in_dim(solved, plane * rows, rows, 2)
    base = jnp.einsum("snr,snp->rp", own_solved, panel_border, preferred_element_type=F32)
    base = base + jnp.where(scen == 0, root_block, 0.0)
    places = part_places(rows).astype(jnp.int32)
    offset = core.reshape(1) * (rows // 2)
    mine, theirs, leading = panel_rows(
        jnp.concatenate([places, offset]), head, base, plane_parts(head)
    )
    panel = mine + swapped(theirs, CORE)
    panel = sum(shifts(panel, "scen_1"))
    panel = sum(shifts(panel, "scen_0"))
    own = plane_parts(panel)
    places = jnp.concatenate([places + offset, places + (rows // 2 - offset)])
    inverse = inverse_factor(places, own + [swapped(part, CORE) for part in own])

    leads = ordered(leading, swapped(leading, CORE), core)
    leads = ordered(*leads, col)
    for slot in range(2):
        bulk = bulk - lax.dot_general(
            slices[:, slot], leads[slot], (((2,), (1,)), ((), ())), preferred_element_type=F32
        )
    pieces = exchanged(bulk.astype(BF16), CHIPS)
    schur = root_block + jnp.sum(pieces.astype(F32), axis=0)
    return lax.dot_general(
        schur, inverse, (((1,), (1,)), ((), ())),
        precision=lax.Precision.HIGH, preferred_element_type=F32,
    )


def solution(mesh):
    split = Mesh(
        mesh.devices.reshape(4, 4, 2, mesh.shape["row"], mesh.shape["col"]),
        ("scen_0", "scen_1", "scen_2", "row", "col"),
    )
    in_specs = (
        P(SCEN, None, ("row", "col"), None),
        P(SCEN, None, None),
        P(SCEN, None, None),
        P(SCEN_ROW, "col"),
        P(SCEN_ROW_COL, None),
    )
    out_specs = P(SCEN_ROW_COL, None)
    return jax.shard_map(
        per_device, mesh=split, in_specs=in_specs, out_specs=out_specs, check_vma=False
    )
```
